32 devices in a mesh: outer: 4 (over x, core), chip: 8 (over z, y).
Axes of the slice: x: 2, y: 2, z: 4, core: 2. Of those that a mesh axis runs over, the one named last changes fastest.
Arguments:
- inputs: bfloat16 [4096, 2048], P(('outer', 'chip')), may hold values from -6 to 6
- out_grads: bfloat16 [4096, 2048], P(('outer', 'chip')), may hold values from -6 to 6
- weight: bfloat16 [2048, 2048], P('chip'), may hold values from -0.125 to 0.125
- start_basis: float32 [64, 2048], P('chip'), may hold values from -6 to 6
- error_buffer: float32 [4, 2048, 2048], P('outer', 'chip'), may hold values from -2 to 2
Outputs:
- outputs: bfloat16 [4096, 2048], P(('outer', 'chip'))
- new_error: float32 [4, 2048, 2048], P('outer', 'chip')
The draws below stay inside these ranges and needn't reach their ends.
All inputs are finite; a program needn't handle non-finite values.
Results may differ from the reference program's by a relative error of at most 0.0085.
Values may be sent and summed in bfloat16 or wider, within the bound.
No kernel may reach another device: no remote copies, remote signals or barrier semaphores. Data moves between devices by JAX's collectives and lax.ppermute only.
A program may use at most 128 MiB of HBM per device.

```python
import jax
import jax.numpy as jnp
from jax import lax

D = 2048
INNER = 2048
RANK = 8
TOK_DEV = 128
PODS = 4
QROWS = 64
TOKENS = 4096
N_CHIP = 8


def block_levels(own_key, extent, shards, least, high):
    def one(position, parts):
        draws = jax.random.uniform(jax.random.fold_in(jax.random.fold_in(own_key, 6), position), (parts,), jnp.float32, least / len(shards), high / len(shards))
        return jnp.repeat(jnp.exp(draws), extent[position] // parts).reshape((-1,) + (1,) * (len(extent) - position - 1))

    factor_of = one(*shards[0])
    for cut in shards[1:]:
        factor_of = factor_of * one(*cut)
    return factor_of


def centred(key, extent, scale, reach, shards=(), kind=jnp.bfloat16):
    level = block_levels(key, extent, shards, -0.22, 0.18) if shards else 1.0
    array = jax.random.normal(key, extent, jnp.float32) * scale * level
    return jnp.minimum(jnp.maximum(array, -reach), reach).astype(kind)


def setup_inputs(seed: int = 0) -> dict:
    keys = jax.random.split(jax.random.key(seed), 6)
    return {
        "inputs": centred(keys[0], (TOKENS, D), 1.0, 6.0, ((0, 32),)),
        "out_grads": centred(keys[1], (TOKENS, INNER), 1.0, 6.0, ((0, 32),)),
        "weight": centred(keys[2], (D, INNER), D ** -0.5, 0.125, ((0, 8),)),
        "start_basis": centred(keys[3], (QROWS, INNER), 1.0, 6.0, ((0, 8),), jnp.float32),
        "error_buffer": centred(keys[4], (PODS, D, INNER), 0.25, 2.0, ((0, 4), (1, 8)), jnp.float32),
    }


LEARNING_RATE = 0.2

def orthonormal(projected):
    finished = []
    for index in range(projected.shape[-2]):
        vector = projected[..., index, :]
        for unit in finished:
            vector = vector - lax.optimization_barrier(jnp.sum(vector * unit, axis=-1, keepdims=True)) * unit
        finished.append(vector / jnp.sqrt(lax.optimization_barrier(jnp.sum(vector * vector, axis=-1, keepdims=True)) + 1.0))
    return jnp.stack(finished, axis=-2)

def reference(inputs, out_grads, weight, start_basis, error_buffer):
    highest = lax.Precision.HIGHEST
    shard_rows = D // N_CHIP
    pod_tokens = TOK_DEV * N_CHIP
    basis_in = start_basis.reshape(N_CHIP, RANK, INNER)
    merged_all = []
    left_sum = jnp.zeros((N_CHIP, RANK, shard_rows), jnp.float32)
    for pod in range(PODS):
        pod_inputs = inputs[pod * pod_tokens:(pod + 1) * pod_tokens]
        pod_grads = out_grads[pod * pod_tokens:(pod + 1) * pod_tokens]
        gradient = lax.dot_general(pod_inputs, pod_grads, (((0,), (0,)), ((), ())), preferred_element_type=jnp.float32) / TOK_DEV
        merged = (gradient + error_buffer[pod]).reshape(N_CHIP, shard_rows, INNER)
        merged_all.append(merged)
        left_sum = left_sum + jnp.einsum('cki,cri->ckr', basis_in, merged, precision=highest)
    left_basis = orthonormal(left_sum / PODS)
    right_sum = jnp.zeros((N_CHIP, RANK, INNER), jnp.float32)
    for merged in merged_all:
        right_sum = right_sum + jnp.einsum('ckr,cri->cki', left_basis, merged, precision=highest)
    right_factor = right_sum / PODS
    approx = jnp.einsum('ckr,cki->cri', left_basis, right_factor, precision=highest)
    new_error = jnp.stack([merged - approx for merged in merged_all]).reshape(PODS, D, INNER)
    new_weight = (weight.astype(jnp.float32) - LEARNING_RATE * approx.reshape(D, INNER)).astype(jnp.bfloat16)
    outputs = jnp.dot(inputs, new_weight, preferred_element_type=jnp.float32).astype(jnp.bfloat16)
    return (outputs, new_error)
```

```python
import functools

import jax
import jax.numpy as jnp
from jax import lax
from jax.experimental import pallas as pl
from jax.experimental.pallas import tpu as pltpu
from jax.sharding import PartitionSpec as P

LEARNING_RATE = 0.2
HIGHEST = lax.Precision.HIGHEST
F32 = jnp.float32
BF16 = jnp.bfloat16


def cycle_of(count):
    minor = 1
    while minor * minor * 4 <= count:
        minor *= 2
    major = count // minor
    if minor < 2 or major % 2 or major * minor != count:
        return list(range(count))
    walk = []
    for row in range(major):
        columns = range(1, minor) if row % 2 == 0 else range(minor - 1, 0, -1)
        walk += [row * minor + column for column in columns]
    return walk + [row * minor for row in reversed(range(major))]


def dot(a, b, dims, precision=None):
    return lax.dot_general(a, b, (dims, ((), ())), precision=precision, preferred_element_type=F32)


NN = ((1,), (0,))
NT = ((1,), (1,))


def call(kernel, outs, args, flops, scalars=0, scratch=()):
    vmem = pl.BlockSpec(memory_space=pltpu.VMEM)
    smem = pl.BlockSpec(memory_space=pltpu.SMEM)
    moved = sum(a.size * a.dtype.itemsize for a in args)
    return pl.pallas_call(
        kernel,
        out_shape=outs,
        in_specs=[smem] * scalars + [vmem] * (len(args) - scalars),
        out_specs=jax.tree.map(lambda _: vmem, outs),
        scratch_shapes=list(scratch),
        cost_estimate=pl.CostEstimate(flops=flops, bytes_accessed=moved, transcendentals=0),
        compiler_params=pltpu.CompilerParams(vmem_limit_bytes=48 * 1024 * 1024),
    )(*args)


def shards(inputs, out_grads, weight, start_basis, error_buffer):
    tokens, depth = inputs.shape
    rows, inner = weight.shape
    rank = start_basis.shape[0]
    n = lax.axis_size("chip")
    pods = lax.axis_size("outer")
    cols = inner // pods
    walk = cycle_of(n)
    place = [walk.index(c) for c in range(n)]
    chip = lax.axis_index("chip")
    outer = lax.axis_index("outer")
    back = jnp.array([[walk[(place[c] - k) % n] for k in range(n)] for c in range(n)], jnp.int32)[chip]
    ahead = jnp.array([[walk[(place[c] + k) % n] for k in range(n)] for c in range(n)], jnp.int32)[chip]

    def shift(value, by):
        return lax.ppermute(value, "chip", [(walk[i], walk[(i + by) % n]) for i in range(n)])

    def swap(value, axis, bit):
        size = lax.axis_size(axis)
        return lax.ppermute(value, axis, [(i, i ^ bit) for i in range(size)])

    pieces = 4
    piece = tokens // pieces

    def split(ahead_ref, x_ref, g_ref, *outs):
        for k in range(n):
            at = pl.multiple_of(ahead_ref[k] * rows, rows)
            outs[k][...] = x_ref[:, pl.ds(at, rows)].T
        for j in range(pieces):
            outs[n + j][...] = g_ref[j * piece : (j + 1) * piece, :]

    parts = call(
        split,
        [jax.ShapeDtypeStruct((rows, tokens), BF16)] * n + [jax.ShapeDtypeStruct((piece, inner), BF16)] * pieces,
        (ahead, inputs, out_grads),
        flops=1000,
        scalars=1,
    )
    x_send, g_now = parts[:n], list(parts[n:])
    x_got = [x_send[0]] + [shift(x_send[k], k) for k in range(1, n)]
    got = {(0, j): g_now[j] for j in range(pieces)}
    mid = None
    for step in range(1, n):
        for j in range(pieces):
            ahead_way = j < pieces // 2
            g_now[j] = shift(g_now[j], 1 if ahead_way else -1)
            got[(step if ahead_way else n - step, j)] = g_now[j]
        if step == n - 2:
            mid = tuple(g_now)
    g_got = [got[(k, j)] for k in range(n) for j in range(pieces)]

    tile = 256

    def merge(basis_ref, err_ref, *refs):
        xs, gs = refs[:n], refs[n : n + n * pieces]
        merged_ref, left_ref, xt, gt = refs[n + n * pieces :]
        for k in range(n):
            xt[:, k * tokens : (k + 1) * tokens] = xs[k][...]
            for j in range(pieces):
                at = k * tokens + j * piece
                gt[at : at + piece, :] = gs[k * pieces + j][...]
        left = jnp.zeros((rank, rows), F32)
        for t in range(inner // tile):
            span = slice(t * tile, (t + 1) * tile)
            part = dot(xt[...], gt[:, span], NN) * (1.0 / tokens) + err_ref[:, span]
            merged_ref[:, span] = part
            left += dot(basis_ref[:, span], part, NT, HIGHEST)
        left_ref[...] = left

    merged, left = call(
        merge,
        (jax.ShapeDtypeStruct((rows, inner), F32), jax.ShapeDtypeStruct((rank, rows), F32)),
        (start_basis, error_buffer[0], *x_got, *g_got),
        flops=2 * rows * inner * n * tokens,
        scratch=(pltpu.VMEM((rows, n * tokens), BF16), pltpu.VMEM((n * tokens, inner), BF16)),
    )

    bits = [1 << i for i in range(pods.bit_length() - 1)] if pods & (pods - 1) == 0 else None
    if bits:
        for bit in bits[:-1]:
            left = left + swap(left, "outer", bit)
        lefts = (left, swap(left, "outer", bits[-1])) if pods > 1 else (left,)
    else:
        lefts = (lax.psum(left, "outer"),)

    def factor(merged_ref, *refs):
        left_refs, (basis_ref, right_ref) = refs[:-2], refs[-2:]
        v = left_refs[0][...]
        for ref in left_refs[1:]:
            v = v + ref[...]
        v = v * (1.0 / pods)
        index = lax.broadcasted_iota(jnp.int32, (rank, 1), 0)
        for k in range(rank - 1):
            row = v[k : k + 1, :]
            along = jnp.sum(v * row, axis=1, keepdims=True)
            scale = along / (along[k : k + 1, :] + 1.0)
            v = v - jnp.where(index > k, scale, 0.0) * row
        basis = v / jnp.sqrt(jnp.sum(v * v, axis=1, keepdims=True) + 1.0)
        basis_ref[...] = basis
        for t in range(inner // tile):
            span = slice(t * tile, (t + 1) * tile)
            right_ref[:, span] = dot(basis, merged_ref[:, span], NN, HIGHEST)

    basis, right = call(
        factor,
        (jax.ShapeDtypeStruct((rank, rows), F32), jax.ShapeDtypeStruct((rank, inner), F32)),
        (merged, *lefts),
        flops=2 * rank * inner * rows * 8,
    )
    if bits:
        for i, bit in enumerate(bits):
            if i:
                right = right.astype(BF16)
            right = right.astype(F32) + swap(right, "outer", bit).astype(F32)
    else:
        right = lax.psum(right.astype(BF16), "outer").astype(F32)
    right = (right * (1.0 / pods)).astype(BF16)
    high = basis.astype(BF16)
    low = (basis - high.astype(F32)).astype(BF16)
    factors = jnp.concatenate([right, high, low], axis=1)

    def residual(merged_ref, basis_ref, right_ref, error_ref):
        basis = basis_ref[...]
        high = basis.astype(BF16)
        rest = basis - high.astype(F32)
        low = rest.astype(BF16)
        least = (rest - low.astype(F32)).astype(BF16)
        stack = jnp.concatenate([high, low, least], axis=0)
        right = right_ref[...]
        thrice = jnp.concatenate([right, right, right], axis=0)
        for t in range(inner // tile):
            span = slice(t * tile, (t + 1) * tile)
            error_ref[:, span] = merged_ref[:, span] - dot(stack, thrice[:, span], ((0,), (0,)))

    new_error = call(
        residual,
        jax.ShapeDtypeStruct((rows, inner), F32),
        (merged, basis, right),
        flops=2 * 3 * rank * inner * rows,
    )[None]

    if n & (n - 1) == 0:
        slots = factors
        bit = 1
        while bit < n:
            slots = jnp.concatenate([slots, swap(slots, "chip", bit)], axis=0)
            bit *= 2
        slot_chip = chip ^ jnp.arange(n, dtype=jnp.int32)
    else:
        slots = lax.all_gather(factors, "chip", axis=0, tiled=True)
        slot_chip = jnp.arange(n, dtype=jnp.int32)

    power = pods & (pods - 1) == 0
    if power:
        hops = [[(i, i ^ k) for i in range(pods)] for k in range(pods)]
        owner = outer ^ jnp.arange(pods, dtype=jnp.int32)
    else:
        hops = [[(i, (i + k) % pods) for i in range(pods)] for k in range(pods)]
        owner = (outer - jnp.arange(pods, dtype=jnp.int32)) % pods
    x_outer = [inputs] + [lax.ppermute(inputs, "outer", hops[k]) for k in range(1, pods)]
    w_own = lax.dynamic_slice_in_dim(weight, outer * cols, cols, axis=1)
    half = rows // 2
    w_now = [w_own[:half], w_own[half:]]
    w_now[0], w_now[1], *_ = lax.optimization_barrier((*w_now, *mid))
    w_got = {(0, j): w_now[j] for j in range(2)}
    for step in range(1, n):
        for j in range(2):
            w_now[j] = shift(w_now[j], 1 if j == 0 else -1)
            w_got[(step if j == 0 else n - step, j)] = w_now[j]

    def product(back_ref, *refs):
        xs, ws, outs = refs[:pods], refs[pods : pods + 2 * n], refs[pods + 2 * n : -2]
        xt, wt = refs[-2:]
        for k in range(n):
            at = pl.multiple_of(back_ref[k] * rows, rows)
            wt[k * rows : k * rows + half, :] = ws[2 * k][...]
            wt[k * rows + half : (k + 1) * rows, :] = ws[2 * k + 1][...]
            for i in range(pods):
                xt[i * tokens : (i + 1) * tokens, k * rows : (k + 1) * rows] = xs[i][:, pl.ds(at, rows)]
        for i in range(pods):
            outs[i][...] = dot(xt[i * tokens : (i + 1) * tokens, :], wt[...], NN).astype(BF16)

    plain = call(
        product,
        [jax.ShapeDtypeStruct((tokens, cols), BF16)] * pods,
        (back, *x_outer, *[w_got[(k, j)] for k in range(n) for j in range(2)]),
        flops=2 * pods * tokens * depth * cols,
        scalars=1,
        scratch=(pltpu.VMEM((pods * tokens, depth), BF16), pltpu.VMEM((depth, cols), BF16)),
    )
    reverse = hops if power else [[(b, a) for a, b in hop] for hop in hops]
    home = [plain[0]] + [lax.ppermute(plain[k], "outer", reverse[k]) for k in range(1, pods)]

    def finish(slot_ref, owner_ref, x_ref, factors_ref, *refs):
        homes, out_ref, corr = refs[:pods], refs[pods], refs[pods + 1]
        columns = []
        for j in range(n):
            at = pl.multiple_of(slot_ref[j] * rows, rows)
            pair = jnp.concatenate(
                [factors_ref[j * rank : (j + 1) * rank, inner : inner + rows],
                 factors_ref[j * rank : (j + 1) * rank, inner + rows :]], axis=0)
            both = dot(x_ref[:, pl.ds(at, rows)], pair, NT)
            columns.append(both[:, :rank] + both[:, rank:])
        inner_factor = jnp.concatenate(columns, axis=1) * LEARNING_RATE
        high = inner_factor.astype(BF16)
        low = (inner_factor - high.astype(F32)).astype(BF16)
        right = factors_ref[:, :inner]
        corr[...] = dot(high, right, NN) + dot(low, right, NN)
        for i in range(pods):
            span = pl.ds(pl.multiple_of(owner_ref[i] * cols, cols), cols)
            out_ref[:, span] = (homes[i][...].astype(F32) - corr[:, span]).astype(BF16)

    outputs = call(
        finish,
        jax.ShapeDtypeStruct((tokens, inner), BF16),
        (slot_chip, owner, inputs, slots, *home),
        flops=4 * tokens * n * rank * inner,
        scalars=2,
        scratch=(pltpu.VMEM((tokens, inner), F32),),
    )
    return outputs, new_error


def solution(mesh):
    return jax.shard_map(
        shards,
        mesh=mesh,
        in_specs=(
            P(("outer", "chip"), None),
            P(("outer", "chip"), None),
            P("chip", None),
            P("chip", None),
            P("outer", "chip", None),
        ),
        out_specs=(P(("outer", "chip"), None), P("outer", "chip", None)),
        check_vma=False,
    )
```
